32 devices in a mesh: dp: 4 (over z), expert: 2 (over y), mp: 4 (over x, core).
Axes of the slice: x: 2, y: 2, z: 4, core: 2. Of those that a mesh axis runs over, the one named last changes fastest.
Arguments:
- tokens: bfloat16 [1024, 2048], P(('dp', 'expert'), 'mp'), may hold values from -6 to 6
- targets: bfloat16 [1024, 2048], P(('dp', 'expert'), 'mp'), may hold values from -6 to 6
- token_weight: float32 [1024], P(('dp', 'expert')), may hold values from 0.5 to 11.7, as said below
- routes: int32 [1024, 2], P(('dp', 'expert')), may hold values from 0 to 7, all different within a row; in each aligned block of 128 rows (0 to 127, 128 to 255, ...) at most 40 rows name the same one
- router_weight: bfloat16 [2048, 8], P('mp'), may hold values from -0.125 to 0.125
- base_weight: bfloat16 [3, 8, 2048, 8192], P(None, 'expert', None, ('dp', 'mp')), may hold values from -0.125 to 0.125
- direction_one: bfloat16 [3, 8, 2048, 8192], P(None, 'expert', None, ('dp', 'mp')), may hold values from -0.125 to 0.125
- direction_two: bfloat16 [3, 8, 2048, 8192], P(None, 'expert', None, ('dp', 'mp')), may hold values from -0.125 to 0.125
- filter_scale: float32 [2, 8, 8192], P(None, 'expert', ('dp', 'mp')), may hold values from 0.5 to 2
- landscape: float32 [2], replicated, may hold values from -0.6 to 0.6
Outputs:
- mixed: bfloat16 [1024, 2048], P(('dp', 'expert'), 'mp')
- loss: float32 [1], replicated
The draws below stay inside these ranges and needn't reach their ends.
Inputs may be any that keep to these rules, and one draw needn't show every extreme that they name: `routes`: each row names 2 different experts. Within the rows of one group of dp and expert (aligned blocks of 128 rows) no expert is named more than 40 times, a bound that some block reaches. `token_weight`: Positive.
All inputs are finite; a program needn't handle non-finite values.
Results may differ from the reference program's by a relative error of at most 0.0028.
The reference program's roundings to bfloat16 on the way count: a program that leaves them out, or rounds other values in their place, can miss the bound.
Values may be sent and summed in bfloat16 or wider, within the bound.
A program may use at most 192 MiB of HBM per device.

```python
import math
import jax
import jax.numpy as jnp
import numpy as np
from jax import lax

D = 2048
FF = 8192
E = 8
TOP = 2
TOK_DEV = 128
CAP = 40
TOKENS = 1024
N_DP = 4
N_EXPERT = 2


def draw_token_weight(key, part):
    position = jnp.arange(TOKENS, dtype=jnp.float32) / TOKENS
    ramp = 1.0 + 2.0 * position
    return ramp * jax.random.uniform(key, (TOKENS,), jnp.float32, 0.5, 1.5)


def shard_levels(stream_key, extent, split, least, top_value):
    factor_of, own = 1.0, jax.random.fold_in(stream_key, 6)
    for dim, shards_of in split:
        draws = jnp.exp(jax.random.uniform(jax.random.fold_in(own, dim), (shards_of,), jnp.float32, least / len(split), top_value / len(split)))
        factor_of = factor_of * jnp.repeat(draws, extent[dim] // shards_of).reshape([-1 if axis == dim else 1 for axis in range(len(extent))])
    return factor_of


def assign_block(own_key, own, number, rows, count, top, reach, skew):
    sequence = jax.random.permutation(own_key, count)
    heavy_load, ordinary = portions_of(count, rows * top, reach, skew, True), portions_of(count, rows * top, reach, skew, False)
    places = jnp.arange(count)

    def named(tallies, offset_by):
        used = int((tallies > 0).sum())
        fixed = max(1, used // 4)
        moved = fixed + (places - fixed + offset_by * (used - fixed)) % max(1, count - fixed)
        return jnp.zeros((count,), jnp.int32).at[sequence[jnp.where(places < fixed, places, moved)]].set(jnp.asarray(tallies, jnp.int32))

    tallies = jnp.where(number % 4 == 0, named(heavy_load, number // 4), named(ordinary, number - number // 4 - 1))
    mixed = jax.random.permutation(jax.random.fold_in(own, 3), count)
    donor, sink = mixed[0:count // 2 * 2:2], mixed[1:count // 2 * 2:2]
    slack = jnp.minimum(tallies[donor] - 1, reach - tallies[sink]) // 2
    slack = jnp.where((donor == sequence[0]) | (sink == sequence[0]) | (tallies[sink] == 0), 0, jnp.maximum(slack, 0))
    moved = jax.random.randint(jax.random.fold_in(own, 4), (count // 2,), 0, 1 << 20) % (slack + 1)
    tallies = tallies.at[donor].add(-moved).at[sink].add(moved)
    items = jnp.searchsorted(jnp.cumsum(tallies), jnp.arange(rows * top), side="right").astype(jnp.int32)
    listing = items.reshape(top, rows).T
    listing = listing[jax.random.permutation(jax.random.fold_in(own, 1), rows)]
    offset_by = jax.random.randint(jax.random.fold_in(own, 2), (rows, 1), 0, top)
    return jnp.take_along_axis(listing, (jnp.arange(top)[None, :] + offset_by) % top, axis=1)


def portions_of(amount, total, reach, lean, full):
    portions = [(1 << 20) // math.isqrt(rank ** lean) + 1 for rank in range(1, amount + 1)]
    largest = reach if full else min(reach, max(-(-total // amount), total * portions[0] // sum(portions)))
    least = 1 if total - largest >= amount - 1 else 0
    counts, spare = [largest] + [least] * (amount - 1), total - largest - least * (amount - 1)
    while spare > 0:
        free = [i for i in range(1, amount) if counts[i] < largest] or [i for i in range(1, amount) if counts[i] < reach]
        whole, remaining = sum([portions[i] for i in free]), spare
        for i in free:
            more = min(reach - counts[i], max(1, remaining * portions[i] // whole), spare)
            counts[i] = counts[i] + more
            spare = spare - more
    return np.array(counts)


def noise(rng, shape, width, limit, split=(), held_as=jnp.bfloat16):
    gain = shard_levels(rng, shape, split, -0.22, 0.18) if split else 1.0
    array = jax.random.normal(rng, shape, jnp.float32) * width * gain
    return jnp.minimum(jnp.maximum(array, -limit), limit).astype(held_as)


def setup_inputs(seed: int = 0) -> dict:
    key_of = jax.random.split(jax.random.key(seed), 11)
    tokens = noise(key_of[0], (TOKENS, D), 1.0, 6.0, ((0, 8), (1, 4)))
    targets = noise(key_of[1], (TOKENS, D), 1.0, 6.0, ((0, 8), (1, 4)))
    token_weight = draw_token_weight(jax.random.fold_in(key_of[10], 71), 0)
    routes_keys = jax.random.split(jax.random.fold_in(key_of[3], 1), TOKENS // TOK_DEV)
    routes_turns = jax.random.permutation(jax.random.fold_in(key_of[3], 3), TOKENS // TOK_DEV)
    routes = jax.vmap(lambda own, number: assign_block(jax.random.fold_in(key_of[3], 2), own, number, TOK_DEV, E, TOP, CAP, 2))(routes_keys, routes_turns).reshape((TOKENS, TOP))
    router_weight = noise(key_of[4], (D, E), D ** -0.5, 0.125, ((0, 4),))
    base_weight = noise(key_of[5], (3, E, D, FF), D ** -0.5, 0.125, ((1, 2), (3, 16)))
    direction_one = noise(key_of[6], (3, E, D, FF), D ** -0.5, 0.125, ((1, 2), (3, 16)))
    direction_two = noise(key_of[7], (3, E, D, FF), D ** -0.5, 0.125, ((1, 2), (3, 16)))
    filter_scale = jnp.clip(jnp.exp(math.log(2.0) - 1.3862944 * jax.random.uniform(key_of[8], (2, E, FF), jnp.float32) ** shard_levels(key_of[8], (2, E, FF), ((1, 2), (2, 16)), -0.2, 0.2)), 0.5, 2.0)
    landscape = jnp.clip(jax.random.uniform(key_of[9], (2,), jnp.float32, -0.6, 0.6), -0.6, 0.6)
    return dict(tokens=tokens, targets=targets, token_weight=token_weight, routes=routes, router_weight=router_weight, base_weight=base_weight, direction_one=direction_one, direction_two=direction_two, filter_scale=filter_scale, landscape=landscape)


def reference(tokens, targets, token_weight, routes, router_weight, base_weight, direction_one, direction_two, filter_scale, landscape):
    groups = N_DP * N_EXPERT
    logits = jnp.dot(tokens, router_weight, preferred_element_type=jnp.float32)
    expert_ids = jnp.arange(E, dtype=jnp.int32)
    pick_first = jnp.sum(jnp.where(routes[:, 0:1] == expert_ids[None, :], logits, jnp.float32(0.0)), axis=1)
    pick_second = jnp.sum(jnp.where(routes[:, 1:2] == expert_ids[None, :], logits, jnp.float32(0.0)), axis=1)
    gate_first = 1.0 / (1.0 + jnp.exp(pick_second - pick_first))
    gate_second = 1.0 / (1.0 + jnp.exp(pick_first - pick_second))
    grouped = routes.reshape(groups, TOK_DEV, 2)
    pair_ids = jnp.concatenate([grouped[:, :, 0], grouped[:, :, 1]], axis=1)
    onehot = (pair_ids[:, :, None] == expert_ids[None, None, :]).astype(jnp.int32)
    earlier = jnp.cumsum(onehot, axis=1) - onehot
    slot = jnp.sum(earlier * onehot, axis=2).astype(jnp.int32)
    flat_index = (pair_ids * CAP + slot).astype(jnp.int32)
    token_groups = tokens.reshape(groups, TOK_DEV, D)
    doubled = jnp.concatenate([token_groups, token_groups], axis=1)
    group_ids = jnp.arange(groups, dtype=jnp.int32)[:, None]
    buffer = jnp.zeros((groups, E * CAP, D), jnp.bfloat16).at[group_ids, flat_index].set(doubled)
    buffer = buffer.reshape(groups, E, CAP, D).transpose(1, 0, 2, 3)

    def run_expert(expert):
        slot_rows = lax.dynamic_index_in_dim(buffer, expert, 0, keepdims=False).reshape(groups * CAP, D)
        base_e = lax.dynamic_index_in_dim(base_weight, expert, 1, keepdims=False)
        one_e = lax.dynamic_index_in_dim(direction_one, expert, 1, keepdims=False)
        two_e = lax.dynamic_index_in_dim(direction_two, expert, 1, keepdims=False)
        scale_e = lax.dynamic_index_in_dim(filter_scale, expert, 1, keepdims=False)
        rebuilt = (base_e.astype(jnp.float32)
                   + landscape[0] * scale_e[0][None, None, :] * one_e.astype(jnp.float32)
                   + landscape[1] * scale_e[1][None, None, :] * two_e.astype(jnp.float32)).astype(jnp.bfloat16)
        gate_value = jnp.dot(slot_rows, rebuilt[0], preferred_element_type=jnp.float32)
        up_value = jnp.dot(slot_rows, rebuilt[1], preferred_element_type=jnp.float32)
        hidden = (jax.nn.silu(gate_value) * up_value).astype(jnp.bfloat16)
        result = jnp.dot(hidden, rebuilt[2].T, preferred_element_type=jnp.float32).astype(jnp.bfloat16)
        return result.reshape(groups, CAP, D)

    expert_out = lax.map(run_expert, jnp.arange(E, dtype=jnp.int32))
    out_flat = expert_out.transpose(1, 0, 2, 3).reshape(groups, E * CAP, D)
    picked = jnp.take_along_axis(out_flat, flat_index[:, :, None], axis=1).astype(jnp.float32)
    first_out = picked[:, :TOK_DEV].reshape(TOKENS, D)
    second_out = picked[:, TOK_DEV:].reshape(TOKENS, D)
    combined = tokens.astype(jnp.float32) + gate_first[:, None] * first_out + gate_second[:, None] * second_out
    error = combined - targets.astype(jnp.float32)
    loss = (jnp.sum(token_weight[:, None] * error * error) / (TOKENS * D)).reshape(1)
    return combined.astype(jnp.bfloat16), loss
```

```python
import jax
import jax.numpy as jnp
from jax import lax
from jax.sharding import PartitionSpec as P

CAP = 40


def rebuild(base_weight, direction_one, direction_two, filter_scale, landscape):
    scale_one = filter_scale[0][None, :, None, :]
    scale_two = filter_scale[1][None, :, None, :]
    merged = (
        base_weight.astype(jnp.float32)
        + landscape[0] * scale_one * direction_one.astype(jnp.float32)
        + landscape[1] * scale_two * direction_two.astype(jnp.float32)
    )
    return merged.astype(jnp.bfloat16)


def slot_target(routes, expert_count, capacity):
    pair_ids = jnp.concatenate([routes[:, 0], routes[:, 1]])
    expert_ids = jnp.arange(expert_count, dtype=jnp.int32)
    onehot = (pair_ids[:, None] == expert_ids[None, :]).astype(jnp.int32)
    earlier = jnp.cumsum(onehot, axis=0) - onehot
    slot = jnp.sum(earlier * onehot, axis=1)
    return pair_ids * capacity + slot


def per_device(
    tokens,
    targets,
    token_weight,
    routes,
    router_weight,
    base_weight,
    direction_one,
    direction_two,
    filter_scale,
    landscape,
):
    tok_rows, feat_local = tokens.shape
    expert_count = router_weight.shape[1]
    local_experts = base_weight.shape[1]
    model_width = base_weight.shape[2]
    hidden_local = base_weight.shape[3]
    expert_devices = lax.axis_size("expert")
    dp_count = lax.axis_size("dp")
    mp_count = lax.axis_size("mp")
    stacked = jnp.concatenate([tokens, router_weight.T], axis=0)
    gathered = lax.all_gather(stacked, "mp", axis=1, tiled=True)
    source = gathered[:tok_rows]
    logits = lax.dot_general(
        source,
        gathered[tok_rows:],
        (((1,), (1,)), ((), ())),
        preferred_element_type=jnp.float32,
    )
    expert_ids = jnp.arange(expert_count, dtype=jnp.int32)
    pick_first = jnp.sum(jnp.where(routes[:, 0:1] == expert_ids[None, :], logits, 0.0), axis=1)
    pick_second = jnp.sum(jnp.where(routes[:, 1:2] == expert_ids[None, :], logits, 0.0), axis=1)
    gate_first = 1.0 / (1.0 + jnp.exp(pick_second - pick_first))
    gate_second = 1.0 / (1.0 + jnp.exp(pick_first - pick_second))
    flat_index = slot_target(routes, expert_count, CAP)
    placer = (
        flat_index[:, None] == jnp.arange(expert_count * CAP, dtype=jnp.int32)[None, :]
    ).astype(jnp.bfloat16)
    doubled = jnp.concatenate([source, source], axis=0)
    buffer = jnp.einsum("pk,pf->kf", placer, doubled, preferred_element_type=jnp.float32).astype(
        jnp.bfloat16
    )
    buffer = buffer.reshape(expert_count, CAP, source.shape[1])
    received = lax.all_to_all(buffer, "expert", split_axis=0, concat_axis=0, tiled=True)
    slots = received.reshape(expert_devices, local_experts, CAP, model_width)
    rebuilt = rebuild(base_weight, direction_one, direction_two, filter_scale, landscape)
    shard_piece = lax.all_gather(slots, "dp", axis=0, tiled=True)
    gate_value = jnp.einsum(
        "njqd,jdh->njqh", shard_piece, rebuilt[0], preferred_element_type=jnp.float32
    )
    up_value = jnp.einsum(
        "njqd,jdh->njqh", shard_piece, rebuilt[1], preferred_element_type=jnp.float32
    )
    hidden = (jax.nn.silu(gate_value) * up_value).astype(jnp.bfloat16)
    hidden_groups = hidden.reshape(dp_count, expert_devices, local_experts, CAP, hidden_local)
    down_blocks = (
        rebuilt[2].reshape(local_experts, mp_count, feat_local, hidden_local).transpose(1, 0, 2, 3)
    )
    partial = jnp.einsum(
        "gnjqh,mjfh->gmnjqf", hidden_groups, down_blocks, preferred_element_type=jnp.float32
    )
    partial = partial.reshape((dp_count * mp_count,) + partial.shape[2:])
    summed = lax.psum_scatter(partial, ("dp", "mp"), scatter_dimension=0, tiled=True)
    expert_out = summed[0].astype(jnp.bfloat16)
    returned = lax.all_to_all(expert_out, "expert", split_axis=0, concat_axis=0, tiled=True)
    out_rows = returned.reshape(expert_count * CAP, feat_local)
    first_out = jnp.take(out_rows, flat_index[:tok_rows], axis=0).astype(jnp.float32)
    second_out = jnp.take(out_rows, flat_index[tok_rows:], axis=0).astype(jnp.float32)
    combined = (
        tokens.astype(jnp.float32)
        + gate_first[:, None] * first_out
        + gate_second[:, None] * second_out
    )
    error = combined - targets.astype(jnp.float32)
    partial_loss = jnp.sum(token_weight[:, None] * error * error)
    loss_total = lax.psum(partial_loss, ("dp", "expert", "mp"))
    entries = tok_rows * dp_count * expert_devices * feat_local * mp_count
    loss = (loss_total / entries).reshape(1)
    return (combined.astype(jnp.bfloat16), loss)


def solution(mesh):
    in_specs = (
        P(("dp", "expert"), "mp"),
        P(("dp", "expert"), "mp"),
        P(("dp", "expert")),
        P(("dp", "expert"), None),
        P("mp", None),
        P(None, "expert", None, ("dp", "mp")),
        P(None, "expert", None, ("dp", "mp")),
        P(None, "expert", None, ("dp", "mp")),
        P(None, "expert", ("dp", "mp")),
        P(),
    )
    out_specs = (P(("dp", "expert"), "mp"), P())
    return jax.shard_map(
        per_device, mesh=mesh, in_specs=in_specs, out_specs=out_specs, check_vma=False
    )
```
